32 devices in a mesh: slab: 8 (over z, y), plane: 4 (over x, core).
Axes of the slice: x: 2, y: 2, z: 4, core: 2. Of those that a mesh axis runs over, the one named last changes fastest.
Arguments:
- a_blocks: bfloat16 [4, 96, 7, 128, 128], P('plane', 'slab'), may hold values from -0.1875 to 0.1875
- a_cols: int32 [4, 96, 7], P('plane', 'slab'), may hold values from 0 to 95, as said below
- p_blocks: bfloat16 [4, 96, 4, 128, 128], P('plane', 'slab'), may hold values from -0.75 to 0.75
- p_cols: int32 [4, 96, 4], replicated, may hold values from 0 to 31, as said below
- coarse_slot: int32 [8, 4], replicated, may hold values from 0 to 3, each once within a row
Outputs:
- coarse_op: float32 [4, 8, 128, 2560], P('plane', 'slab')
The draws below stay inside these ranges and needn't reach their ends.
Inputs may be any that keep to these rules, and one draw needn't show every extreme that they name: `a_cols`: row g = s*12 + r of column p names 7 distinct block rows of column p, among them g itself; they lie in s*12 to s*12 + 11, or, if r < 4, in the 4 rows just below s*12, or, if r >= 8, in the 4 rows from (s+1)*12 on. `p_cols`: row g = s*12 + r names 4 distinct coarse blocks of s*4 to s*4 + 3, or, if r < 4, also of the 4 blocks before, or, if r >= 8, of the 4 blocks after. `coarse_slot`: each row is a permutation of 0 to 3.
All inputs are finite; a program needn't handle non-finite values.
Results may differ from the reference program's by a relative error of at most 0.0029.
Values may be sent and summed in bfloat16 or wider, within the bound.
A program may use at most 192 MiB of HBM per device.

```python
import jax
import jax.numpy as jnp
from jax import lax

B = 128
BR = 12
GHOST = 4
KA = 7
KP = 4
CB = 1
PLANES = 4
SLABS = 8
CS = 4
NBS = 96
WIN = 2560


def draw_a_cols(key, part):
    rows = jnp.arange(NBS, dtype=jnp.int32)
    slab = rows // BR
    inner = rows % BR
    cand = jnp.arange(BR + 2 * GHOST, dtype=jnp.int32)
    own = (cand[None, :] >= GHOST) & (cand[None, :] < GHOST + BR)
    lower = (cand[None, :] < GHOST) & (inner[:, None] < GHOST) & (slab[:, None] > 0)
    upper = (cand[None, :] >= GHOST + BR) & (inner[:, None] >= BR - GHOST) & (slab[:, None] < SLABS - 1)
    valid = own | lower | upper
    noise = jax.random.randint(key, (PLANES, NBS, BR + 2 * GHOST), 0, 2 ** 20, dtype=jnp.int32)
    score = noise * 128 + cand[None, None, :]
    score = score + jnp.where(lower | upper, 2 ** 27, 0)[None]
    score = score + jnp.where(cand[None, :] == GHOST + inner[:, None], 2 ** 29, 0)[None]
    score = jnp.where(valid[None], score, -1)
    picked = lax.top_k(score, KA)[1].astype(jnp.int32)
    return (slab[None, :, None] * BR - GHOST + picked).astype(jnp.int32)


def draw_p_cols(key, part):
    rows = jnp.arange(NBS, dtype=jnp.int32)
    slab = rows // BR
    inner = rows % BR
    cand = jnp.arange(3 * CS, dtype=jnp.int32)
    own = (cand[None, :] >= CS) & (cand[None, :] < 2 * CS)
    lower = (cand[None, :] < CS) & (inner[:, None] < GHOST) & (slab[:, None] > 0)
    upper = (cand[None, :] >= 2 * CS) & (inner[:, None] >= BR - GHOST) & (slab[:, None] < SLABS - 1)
    valid = own | lower | upper
    noise = jax.random.randint(key, (PLANES, NBS, 3 * CS), 0, 2 ** 20, dtype=jnp.int32)
    score = jnp.where(valid[None], noise * 64 + cand[None, None, :], -1)
    picked = lax.top_k(score, KP)[1].astype(jnp.int32)
    return ((slab[None, :, None] - 1) * CS + picked).astype(jnp.int32)


def shard_levels(key, extent, split, least, high):
    loudness, own = 1.0, jax.random.fold_in(key, 6)
    for dim, blocks in split:
        heights = jnp.exp(jax.random.uniform(jax.random.fold_in(own, dim), (blocks,), jnp.float32, least / len(split), high / len(split)))
        loudness = loudness * jnp.repeat(heights, extent[dim] // blocks).reshape([-1 if axis == dim else 1 for axis in range(len(extent))])
    return loudness


def bell_draw(own_key, dims, scale, bound, shards=(), held_as=jnp.bfloat16):
    array = scale * jax.random.normal(own_key, dims, jnp.float32)
    if shards:
        array = array * shard_levels(own_key, dims, shards, -0.22, 0.18)
    return jnp.clip(array, -bound, bound).astype(held_as)


def setup_inputs(seed: int = 0) -> dict:
    arg_keys = jax.random.split(jax.random.key(seed), 6)
    a_blocks = bell_draw(arg_keys[0], (PLANES, NBS, KA, B, B), (B * KA) ** -0.5, 0.1875, ((0, 4), (1, 8)))
    a_cols = draw_a_cols(jax.random.fold_in(arg_keys[5], 71), 0)
    p_blocks = bell_draw(arg_keys[2], (PLANES, NBS, KP, B, B), 0.125, 0.75, ((0, 4), (1, 8)))
    p_cols = draw_p_cols(jax.random.fold_in(arg_keys[5], 71), 0)
    coarse_slot = jax.vmap(lambda own: jax.random.permutation(own, CS))(jax.random.split(arg_keys[4], SLABS)).reshape((SLABS, CS)).astype(jnp.int32)
    return {"a_blocks": a_blocks, "a_cols": a_cols, "p_blocks": p_blocks, "p_cols": p_cols, "coarse_slot": coarse_slot}


def window_rows(blocks, cols, slot_table, slab):
    count = blocks.shape[0]
    owner = jnp.clip(cols // CS, 0, SLABS - 1)
    inside = cols % CS
    slot = slot_table[owner, inside]
    place = (cols // CS - slab + 1) * CS + slot
    onehot = (place[:, :, None] == jnp.arange(3 * CS, dtype=jnp.int32)[None, None, :]).astype(jnp.float32)
    dense = jnp.einsum('nkw,nkab->nawb', onehot, blocks.astype(jnp.float32))
    return dense.reshape(count, B, 3 * CS * B).astype(jnp.bfloat16)


def reference(a_blocks, a_cols, p_blocks, p_cols, coarse_slot):
    width = 3 * CS * B
    p_padded = jnp.pad(p_blocks, ((0, 0), (GHOST, GHOST), (0, 0), (0, 0), (0, 0)))
    c_padded = jnp.pad(p_cols, ((0, 0), (GHOST, GHOST), (0, 0)))

    def slab_part(slab):
        start = (slab * BR).astype(jnp.int32)
        near_blocks = lax.dynamic_slice_in_dim(p_padded, start, BR + 2 * GHOST, 1)
        near_cols = lax.dynamic_slice_in_dim(c_padded, start, BR + 2 * GHOST, 1)
        dense = window_rows(near_blocks.reshape(-1, KP, B, B), near_cols.reshape(-1, KP), coarse_slot, slab)
        dense = dense.reshape(PLANES, BR + 2 * GHOST, B, width)
        own_a = lax.dynamic_slice_in_dim(a_blocks, start, BR, 1)
        local = lax.dynamic_slice_in_dim(a_cols, start, BR, 1) - (start - GHOST)
        total = jnp.zeros((PLANES, BR, B, width), jnp.float32)
        for k in range(KA):
            picked = jax.vmap(lambda d, i: d[i])(dense, local[:, :, k])
            total = total + jnp.einsum('prab,prbw->praw', own_a[:, :, k].astype(jnp.float32), picked.astype(jnp.float32))
        product = total.astype(jnp.bfloat16)
        own_rows = dense[:, GHOST:GHOST + BR].reshape(-1, width)
        return lax.dot_general(own_rows, product.reshape(-1, width), (((0,), (0,)), ((), ())), preferred_element_type=jnp.float32)

    parts = lax.map(slab_part, jnp.arange(SLABS, dtype=jnp.int32))
    groups = parts.reshape(SLABS, 3, CS * B, width)
    middle = groups[:, 1]
    empty = jnp.zeros((1, CS * B, width), jnp.float32)
    below = jnp.concatenate([empty, groups[:-1, 2]], axis=0)
    above = jnp.concatenate([groups[1:, 0], empty], axis=0)
    edge = CS * B
    full = jnp.pad(middle, ((0, 0), (0, 0), (edge, edge)))
    full = full + jnp.pad(below, ((0, 0), (0, 0), (0, 2 * edge)))
    full = full + jnp.pad(above, ((0, 0), (0, 0), (2 * edge, 0)))
    full = full.reshape(SLABS, PLANES, CB, B, WIN)
    return jnp.transpose(full, (1, 0, 2, 3, 4)).reshape(PLANES, SLABS * CB, B, WIN)
```

```python
import functools

import jax
import jax.numpy as jnp
from jax import lax
from jax.experimental import pallas as pl
from jax.experimental.pallas import tpu as pltpu
from jax.sharding import PartitionSpec as P

GHOST = 4
MESH = pl.DeviceIdType.MESH


def kernel(dims, a_cols_hbm, p_cols_hbm, slots_hbm, a_hbm, p_hbm, out, *scratch):
    slabs, planes, rows, links, kp, block, coarse, owned = dims
    stages = planes.bit_length() - 1
    edge = coarse * block
    chunks = 3
    ghosts = GHOST * kp
    (a_own, p_own, p_low, p_high, q0, q1, q2, qt0, qt1, qt2, dense, dense_low, dense_high, ap, keep_ap, final,
     send_c, recv_c, local_sem, halo_send, halo_recv, c_sem, c_got, whole, out_sem, a_cols, p_cols, slots,
     index_sem) = scratch[:29]
    rest = scratch[29:]
    send_b, recv_b, keep_b, b_sem, b_got = (rest[i * stages : (i + 1) * stages] for i in range(5))
    slab = lax.axis_index("slab")
    me = lax.axis_index("plane")
    bits = [(me // (1 << t)) % 2 for t in range(stages)]
    partners = [me + (1 - 2 * bits[t]) * (1 << t) for t in range(stages)]
    has_low = slab > 0
    has_high = slab < slabs - 1
    f32, bf = jnp.float32, jnp.bfloat16
    start = slab * rows
    total = p_cols.shape[2]
    dot = functools.partial(jnp.dot, preferred_element_type=f32)

    copy_index = [
        pltpu.make_async_copy(source, target, index_sem.at[i])
        for i, (source, target) in enumerate(
            ((a_cols_hbm, a_cols), (p_cols_hbm, p_cols), (slots_hbm, slots)))
    ]
    spans = ((rows - GHOST, GHOST), (0, GHOST), (GHOST, rows - 2 * GHOST))
    copy_p = [
        pltpu.make_async_copy(
            p_hbm.at[pl.ds(first * kp, count * kp)], p_own.at[pl.ds(first * kp, count * kp)], local_sem.at[1 + i])
        for i, (first, count) in enumerate(spans)
    ]
    copy_a = pltpu.make_async_copy(a_hbm, a_own.at[pl.ds(0, rows * links)], local_sem.at[0])
    copy_p[0].start()
    for copy in copy_index:
        copy.start()
    for copy in copy_p[1:]:
        copy.start()
    copy_a.start()

    barrier = pltpu.get_barrier_semaphore()
    for t in range(stages):
        pl.semaphore_signal(barrier, inc=1, device_id=(slab, partners[t]), device_id_type=MESH)

    @pl.when(has_low)
    def _():
        pl.semaphore_signal(barrier, inc=1, device_id=(slab - 1, me), device_id_type=MESH)

    @pl.when(has_high)
    def _():
        pl.semaphore_signal(barrier, inc=1, device_id=(slab + 1, me), device_id_type=MESH)

    zero = jnp.zeros((block, block), bf)
    a_own[rows * links] = zero
    p_own[rows * kp] = zero
    p_low[ghosts] = zero
    p_high[ghosts] = zero

    @pl.when(slab == 0)
    def _():
        p_low[...] = jnp.zeros_like(p_low)
        recv_c[1] = jnp.zeros(recv_c.shape[1:], recv_c.dtype)

    @pl.when(slab == slabs - 1)
    def _():
        p_high[...] = jnp.zeros_like(p_high)
        recv_c[0] = jnp.zeros(recv_c.shape[1:], recv_c.dtype)

    neighbours = stages + jnp.where(has_low, 1, 0) + jnp.where(has_high, 1, 0)
    pl.semaphore_wait(barrier, neighbours)
    copy_p[0].wait()

    halo_up = pltpu.make_async_remote_copy(
        src_ref=p_own.at[pl.ds((rows - GHOST) * kp, ghosts)],
        dst_ref=p_low.at[pl.ds(0, ghosts)],
        send_sem=halo_send.at[0], recv_sem=halo_recv.at[0],
        device_id=(slab + 1, me), device_id_type=MESH)
    halo_down = pltpu.make_async_remote_copy(
        src_ref=p_own.at[pl.ds(0, ghosts)],
        dst_ref=p_high.at[pl.ds(0, ghosts)],
        send_sem=halo_send.at[1], recv_sem=halo_recv.at[1],
        device_id=(slab - 1, me), device_id_type=MESH)

    @pl.when(has_high)
    def _():
        halo_up.start()

    for copy in copy_index:
        copy.wait()

    def find(n, base, none, which):
        row = jnp.clip(start - GHOST + n, 0, total - 1)
        place = []
        for m in range(kp):
            col = p_cols[me, m, row]
            near = col // coarse
            place.append((near - slab + 1) * coarse + slots[col % coarse, near])
        found = []
        for w in which:
            value = none
            for m in range(kp):
                value = jnp.where(place[m] == w, base + m, value)
            found.append(value)
        return found

    def at(i):
        return pl.ds(pl.multiple_of(i * block, block), block)

    middle = range(coarse, 2 * coarse)
    lower = range(0, coarse)
    upper = range(2 * coarse, 3 * coarse)
    q_at = {0: (q0, 0), 1: (q1, 0), 2: (q2, rows)}
    turned = {0: (qt0, 0), 1: (qt1, 0), 2: (qt2, rows - GHOST)}
    half = planes // 2

    def spread(first, count, which, blocks, offset, none, turn):
        def body(i, _):
            n = first + i
            found = find(n, (n - offset) * kp, none, which)
            for w, value in zip(which, found):
                j, slot = w // coarse, w % coarse
                q, before = q_at[j]
                piece = blocks[value]
                q[at(n - before), slot * block : (slot + 1) * block] = piece
                if turn:
                    qt, base = turned[j]
                    owner = slot // owned
                    low = (owner // 2) * owned * block + (slot % owned) * block
                    qt[owner % 2, low : low + block, at(n - GHOST - base)] = piece.T
            return 0

        lax.fori_loop(0, count, body, 0)

    for copy in copy_p[1:]:
        copy.wait()
    none = rows * kp
    spread(GHOST, GHOST, [*lower, *middle], p_own, GHOST, none, True)
    spread(2 * GHOST, rows - 2 * GHOST, [*middle], p_own, GHOST, none, True)
    spread(rows, GHOST, [*middle, *upper], p_own, GHOST, none, True)
    copy_a.wait()

    def place(first, count, low, high):
        def body(i, _):
            g = first + i
            local = [a_cols[k, 0, g] - (start - GHOST) for k in range(links)]
            for n in range(low, high):
                value = rows * links
                for k in range(links):
                    value = jnp.where(local[k] == n, g * links + k, value)
                piece = a_own[value]
                if n < GHOST:
                    dense_low[at(g), n * block : (n + 1) * block] = piece
                elif n < GHOST + rows:
                    dense[at(g), (n - GHOST) * block : (n - GHOST + 1) * block] = piece
                else:
                    m = n - GHOST - rows
                    dense_high[at(g - rows + GHOST), m * block : (m + 1) * block] = piece
            return 0

        lax.fori_loop(0, count, body, 0)

    place(0, GHOST, 0, GHOST + rows)
    place(GHOST, rows - 2 * GHOST, GHOST, GHOST + rows)
    place(rows - GHOST, GHOST, GHOST, rows + 2 * GHOST)

    gb = GHOST * block
    rb = rows * block
    bands = ((0, gb), (gb, rb - gb), (rb - gb, rb))
    inner = {0: (0, gb), 1: (0, rb), 2: (rb - gb, rb)}

    def own(band, c):
        first, last = bands[band]
        k0, k1 = inner[c]
        q, before = q_at[c]
        shift = gb - before * block
        keep = {(0, 0): 0, (0, 1): 1, (2, 1): 2, (2, 2): 3}.get((band, c))
        step = min(2 * block, last - first)
        for m in range(first, last, step):
            value = dot(dense[m : m + step, k0:k1], q[k0 + shift : k1 + shift, :])
            if keep is None:
                ap[c, m : m + step, :] = value.astype(bf)
            else:
                keep_ap[keep, m - first : m - first + step, :] = value

    def ghost(band, c):
        first, last = bands[band]
        q, before = q_at[c]
        left = dense_low if band == 0 else dense_high
        shift = (0 if band == 0 else gb + rb) - before * block
        keep = {(0, 0): 0, (0, 1): 1, (2, 1): 2, (2, 2): 3}[(band, c)]
        step = 2 * block
        for m in range(0, gb, step):
            value = dot(left[m : m + step, :], q[shift : shift + gb, :])
            ap[c, first + m : first + m + step, :] = (keep_ap[keep, m : m + step, :] + value).astype(bf)

    def stage_copy(t, j, c):
        return pltpu.make_async_remote_copy(
            src_ref=send_b[t].at[j, c], dst_ref=recv_b[t].at[j, c],
            send_sem=b_sem[t].at[j, c], recv_sem=b_got[t].at[j, c],
            device_id=(slab, partners[t]), device_id_type=MESH)

    def final_copy(j, c):
        return pltpu.make_async_remote_copy(
            src_ref=send_c.at[j, c], dst_ref=recv_c.at[j, c],
            send_sem=c_sem.at[j, c], recv_sem=c_got.at[j, c],
            device_id=(slab - 1 if j == 0 else slab + 1, me), device_id_type=MESH)

    parts = ((qt0, 0, gb), (qt1, 0, rb), (qt2, rb - gb, gb))
    shape = (half, owned * block, edge)

    def form(j, c):
        qt, first, depth = parts[j]
        right = ap[c, first : first + depth, :]
        send_b[0][j, c] = dot(qt[1 - bits[0]], right).astype(bf).reshape(shape)
        stage_copy(0, j, c).start()
        keep_b[0][j, c] = dot(qt[bits[0]], right).reshape(shape)

    def fold(j, c):
        for t in range(1, stages):
            stage_copy(t - 1, j, c).wait_recv()
            for i in range(planes >> (t + 1)):
                k = 1 - bits[t] + 2 * i
                send_b[t][j, c, i] = (
                    keep_b[t - 1][j, c, k] + recv_b[t - 1][j, c, k].astype(f32)).astype(bf)
            stage_copy(t, j, c).start()
            for i in range(planes >> (t + 1)):
                k = bits[t] + 2 * i
                keep_b[t][j, c, i] = keep_b[t - 1][j, c, k] + recv_b[t - 1][j, c, k].astype(f32)

    def finish(j, c):
        stage_copy(stages - 1, j, c).wait_recv()
        value = keep_b[stages - 1][j, c, 0] + recv_b[stages - 1][j, c, 0].astype(f32)
        if j == 1:
            final[c] = value
        else:
            send_c[j // 2, c] = value.astype(bf)

    def send(j, c):
        @pl.when(has_low if j == 0 else has_high)
        def _():
            final_copy(j // 2, c).start()

    own(0, 2)
    form(0, 2)
    own(2, 0)
    form(2, 0)
    own(0, 0)
    own(0, 1)
    fold(0, 2)
    fold(2, 0)
    own(1, 1)
    own(1, 0)
    own(1, 2)

    @pl.when(has_high)
    def _():
        halo_up.wait_send()

    @pl.when(has_low)
    def _():
        halo_down.start()

    own(2, 2)
    own(2, 1)

    @pl.when(has_low)
    def _():
        halo_up.wait_recv()

    spread(0, GHOST, [*lower, *middle], p_low, 0, ghosts, False)
    ghost(0, 0)
    form(0, 0)
    ghost(0, 1)
    form(0, 1)
    form(1, 0)
    fold(0, 0)
    fold(0, 1)
    fold(1, 0)
    finish(0, 2)
    finish(2, 0)
    finish(0, 0)

    @pl.when(has_low)
    def _():
        halo_down.wait_send()

    send(0, 2)
    send(2, 0)
    send(0, 0)
    finish(0, 1)
    send(0, 1)

    @pl.when(has_high)
    def _():
        halo_down.wait_recv()

    spread(GHOST + rows, GHOST, [*middle, *upper], p_high, GHOST + rows, ghosts, False)
    ghost(2, 1)
    form(2, 1)
    ghost(2, 2)
    form(2, 2)
    fold(2, 1)
    fold(2, 2)
    form(1, 2)
    form(1, 1)
    fold(1, 2)
    fold(1, 1)
    finish(2, 1)
    send(2, 1)
    finish(2, 2)
    send(2, 2)
    finish(1, 0)
    finish(1, 2)
    finish(1, 1)

    def out_copy(o):
        return pltpu.make_async_copy(whole.at[o], out.at[:, pl.ds(o * edge, edge)], out_sem.at[o])

    for o in (4, 3, 2, 1, 0):
        terms = []
        if 0 <= o - 1 < chunks:
            terms.append(final[o - 1])
        if o >= 2:
            @pl.when(has_high)
            def _():
                final_copy(0, o - 2).wait_recv()

            terms.append(recv_c[0, o - 2].astype(f32))
        if o < chunks:
            @pl.when(has_low)
            def _():
                final_copy(1, o).wait_recv()

            terms.append(recv_c[1, o].astype(f32))
        whole[o] = functools.reduce(jnp.add, terms)
        out_copy(o).start()

    @pl.when(has_high)
    def _():
        for c in range(chunks):
            final_copy(1, c).wait_send()

    @pl.when(has_low)
    def _():
        for c in range(chunks):
            final_copy(0, c).wait_send()

    for t in range(stages):
        for j in range(3):
            for c in range(chunks):
                stage_copy(t, j, c).wait_send()
    for o in range(5):
        out_copy(o).wait()


def on_device(a_blocks, a_cols, p_blocks, p_cols, coarse_slot):
    rows, links, block = a_blocks.shape[1:4]
    kp = p_blocks.shape[2]
    coarse = coarse_slot.shape[1]
    slabs = lax.axis_size("slab")
    planes = lax.axis_size("plane")
    owned = coarse // planes
    stages = planes.bit_length() - 1
    assert planes == 1 << stages and stages > 0 and rows >= 2 * GHOST
    edge = coarse * block
    high = owned * block
    dims = (slabs, planes, rows, links, kp, block, coarse, owned)
    bf, f32 = jnp.bfloat16, jnp.float32
    vmem = pltpu.VMEM
    dma = pltpu.SemaphoreType.DMA
    gb, rb = GHOST * block, rows * block
    shape = lambda t: (3, 3, planes >> (t + 1), high, edge)
    scratch = [
        vmem((rows * links + 1, block, block), bf),
        vmem((rows * kp + 1, block, block), bf),
        vmem((GHOST * kp + 1, block, block), bf),
        vmem((GHOST * kp + 1, block, block), bf),
        vmem((2 * gb, edge), bf),
        vmem((rb + 2 * gb, edge), bf),
        vmem((2 * gb, edge), bf),
        vmem((2, planes // 2 * high, gb), bf),
        vmem((2, planes // 2 * high, rb), bf),
        vmem((2, planes // 2 * high, gb), bf),
        vmem((rb, rb), bf),
        vmem((gb, gb), bf),
        vmem((gb, gb), bf),
        vmem((3, rb, edge), bf),
        vmem((4, gb, edge), f32),
        vmem((3, high, edge), f32),
        vmem((2, 3, high, edge), bf),
        vmem((2, 3, high, edge), bf),
        dma((4,)), dma((2,)), dma((2,)), dma((2, 3)), dma((2, 3)),
        vmem((5, high, edge), f32),
        dma((5,)),
        pltpu.SMEM((links, 1, rows), jnp.int32),
        pltpu.SMEM((planes, kp, p_cols.shape[1]), jnp.int32),
        pltpu.SMEM((coarse, slabs), jnp.int32),
        dma((3,)),
    ]
    scratch += [vmem(shape(t), bf) for t in range(stages)]
    scratch += [vmem(shape(t), bf) for t in range(stages)]
    scratch += [vmem(shape(t), f32) for t in range(stages)]
    scratch += [dma((3, 3)) for t in range(2 * stages)]
    outside = pl.BlockSpec(memory_space=pltpu.HBM)
    anywhere = pl.BlockSpec(memory_space=pl.ANY)
    result = pl.pallas_call(
        functools.partial(kernel, dims),
        out_shape=jax.ShapeDtypeStruct((high, 5 * edge), f32),
        in_specs=[outside] * 5,
        out_specs=anywhere,
        scratch_shapes=scratch,
        compiler_params=pltpu.CompilerParams(
            collective_id=0, has_side_effects=True, vmem_limit_bytes=50 * 1024 * 1024),
    )(*(pltpu.with_memory_space_constraint(x, pltpu.HBM) for x in (
        a_cols.transpose(2, 0, 1), p_cols.transpose(0, 2, 1), coarse_slot.T,
        a_blocks.reshape(rows * links, block, block), p_blocks.reshape(rows * kp, block, block))))
    return result.reshape(1, owned, block, 5 * edge)


def solution(mesh):
    return jax.shard_map(
        on_device,
        mesh=mesh,
        in_specs=(
            P("plane", "slab", None, None, None),
            P("plane", "slab", None),
            P("plane", "slab", None, None, None),
            P(),
            P(),
        ),
        out_specs=P("plane", "slab", None, None),
        check_vma=False,
    )
```

```python
import functools

import jax
import jax.numpy as jnp
from jax import lax
from jax.experimental import pallas as pl
from jax.experimental.pallas import tpu as pltpu
from jax.sharding import PartitionSpec as P

GHOST = 4
MESH = pl.DeviceIdType.MESH


def kernel(dims, a_cols_hbm, p_cols_hbm, slots_hbm, a_hbm, p_hbm, out, *scratch):
    slabs, planes, rows, links, kp, block, coarse, owned = dims
    stages = planes.bit_length() - 1
    edge = coarse * block
    chunks = 3
    ghosts = GHOST * kp
    (a_own, p_own, p_low, p_high, q0, q1, q2, qt0, qt1, qt2, dense, dense_low, dense_high, ap, keep_ap, final,
     send_c, recv_c, local_sem, halo_send, halo_recv, c_sem, c_got, whole, out_sem, a_cols, p_cols, slots,
     index_sem, pass_p, pass_c, pass_sem, pass_got, pass_c_sem, pass_c_got) = scratch[:35]
    rest = scratch[35:]
    send_b, recv_b, keep_b, b_sem, b_got = (rest[i * stages : (i + 1) * stages] for i in range(5))
    slab = lax.axis_index("slab")
    me = lax.axis_index("plane")
    bits = [(me // (1 << t)) % 2 for t in range(stages)]
    partners = [me + (1 - 2 * bits[t]) * (1 << t) for t in range(stages)]
    f32, bf = jnp.float32, jnp.bfloat16
    start = slab * rows
    total = p_cols.shape[2]
    dot = functools.partial(jnp.dot, preferred_element_type=f32)
    turn = slab % 2
    pairs = max(slabs // 2, 1)
    level = slab // 2
    first = slab - 1 + 2 * turn
    second = slab + 1 - 2 * turn
    past = slab + 2 - 4 * turn
    has_first = (first >= 0) & (first < slabs)
    has_second = second < slabs
    has_past = (past >= 0) & (past < slabs) & has_second
    far = jnp.where(has_second, jnp.where(turn == 0, level, pairs - 1 - level), 0)
    near = jnp.where(turn == 0, pairs - 1 - level, level)
    opening = turn * (rows - GHOST)
    closing = (1 - turn) * (rows - GHOST)

    def inner_row(i):
        return jnp.where(i < GHOST, opening + i, jnp.where(i < rows - GHOST, i, closing + i - (rows - GHOST)))

    def local_row(n):
        low = jnp.where(turn == 0, n, rows + GHOST + n)
        high = jnp.where(turn == 0, n, n - rows - GHOST)
        return jnp.where(n < GHOST, low, jnp.where(n < GHOST + rows, GHOST + inner_row(n - GHOST), high))

    copy_index = [
        pltpu.make_async_copy(source, target, index_sem.at[i])
        for i, (source, target) in enumerate(
            ((a_cols_hbm, a_cols), (p_cols_hbm, p_cols), (slots_hbm, slots)))
    ]
    spans = ((opening, GHOST), (closing, GHOST), (GHOST, rows - 2 * GHOST))
    copy_p = [
        pltpu.make_async_copy(
            p_hbm.at[pl.ds(head * kp, count * kp)], p_own.at[pl.ds(head * kp, count * kp)], local_sem.at[1 + i])
        for i, (head, count) in enumerate(spans)
    ]
    copy_a = pltpu.make_async_copy(a_hbm, a_own.at[pl.ds(0, rows * links)], local_sem.at[0])
    copy_p[0].start()
    for copy in copy_index:
        copy.start()
    for copy in copy_p[1:]:
        copy.start()
    copy_a.start()

    barrier = pltpu.get_barrier_semaphore()
    for t in range(stages):
        pl.semaphore_signal(barrier, inc=1, device_id=(slab, partners[t]), device_id_type=MESH)

    known = ((slab >= 1, slab - 1), (slab + 1 < slabs, slab + 1), (slab >= 2, slab - 2), (slab + 2 < slabs, slab + 2))
    for exists, device in known:
        @pl.when(exists)
        def _():
            pl.semaphore_signal(barrier, inc=1, device_id=(device, me), device_id_type=MESH)

    zero = jnp.zeros((block, block), bf)
    a_own[rows * links] = zero
    p_own[rows * kp] = zero
    p_low[ghosts] = zero
    p_high[ghosts] = zero

    @pl.when(~has_first)
    def _():
        p_low[...] = jnp.zeros_like(p_low)
        recv_c[0] = jnp.zeros(recv_c.shape[1:], recv_c.dtype)

    @pl.when(~has_second)
    def _():
        p_high[...] = jnp.zeros_like(p_high)
        recv_c[1] = jnp.zeros(recv_c.shape[1:], recv_c.dtype)

    pl.semaphore_wait(barrier, stages + sum(jnp.where(exists, 1, 0) for exists, _ in known))
    copy_p[0].wait()

    sides = ((opening, p_low, first, has_first), (closing, p_high, second, has_second))

    def through(k, i, units):
        return i < k * units // pairs

    def row_copy(o, i, relayed):
        head, target, device, _ = sides[o]
        return pltpu.make_async_remote_copy(
            src_ref=p_own.at[pl.ds((head + i) * kp, kp)],
            dst_ref=(pass_p if relayed else target).at[pl.ds(i * kp, kp)],
            send_sem=halo_send.at[o, i], recv_sem=(pass_got.at[i] if relayed else halo_recv.at[o, i]),
            device_id=(second if relayed else device, me), device_id_type=MESH)

    def pass_copy(i):
        return pltpu.make_async_remote_copy(
            src_ref=pass_p.at[pl.ds(i * kp, kp)], dst_ref=p_low.at[pl.ds(i * kp, kp)],
            send_sem=pass_sem.at[i], recv_sem=halo_recv.at[0, i],
            device_id=(past, me), device_id_type=MESH)

    def halo_start(o):
        exists = sides[o][3]
        for i in range(GHOST):
            direct = exists
            if o == 0 and i < GHOST - 1:
                direct = exists & ~through(far, i, GHOST)

                @pl.when(exists & through(far, i, GHOST))
                def _():
                    row_copy(o, i, True).start()

            @pl.when(direct)
            def _():
                row_copy(o, i, False).start()

    def halo_sent(o):
        @pl.when(sides[o][3])
        def _():
            for i in range(GHOST):
                row_copy(o, i, False).wait_send()

    def halo_pass(i):
        @pl.when(has_past & through(near, i, GHOST))
        def _():
            row_copy(0, i, True).wait_recv()
            pass_copy(i).start()

    def halo_wait(o):
        @pl.when(sides[o][3])
        def _():
            for i in range(GHOST):
                row_copy(o, i, False).wait_recv()

    halo_start(0)

    for copy in copy_index:
        copy.wait()

    def find(n, base, none, which):
        row = jnp.clip(start - GHOST + local_row(n), 0, total - 1)
        place = []
        for m in range(kp):
            col = p_cols[me, m, row]
            ahead = col // coarse
            place.append((1 + (ahead - slab) * (1 - 2 * turn)) * coarse + slots[col % coarse, ahead])
        found = []
        for w in which:
            value = none
            for m in range(kp):
                value = jnp.where(place[m] == w, base + m, value)
            found.append(value)
        return found

    def at(i):
        return pl.ds(pl.multiple_of(i * block, block), block)

    middle = range(coarse, 2 * coarse)
    lower = range(0, coarse)
    upper = range(2 * coarse, 3 * coarse)
    q_at = {0: (q0, 0), 1: (q1, 0), 2: (q2, rows)}
    turned = {0: (qt0, 0), 1: (qt1, 0), 2: (qt2, rows - GHOST)}
    half = planes // 2

    def spread(head, count, which, blocks, none, flip):
        def body(i, _):
            n = head + i
            found = find(n, (inner_row(n - GHOST) if flip else i) * kp, none, which)
            for w, value in zip(which, found):
                j, slot = w // coarse, w % coarse
                q, before = q_at[j]
                piece = blocks[value]
                q[at(n - before), slot * block : (slot + 1) * block] = piece
                if flip:
                    qt, base = turned[j]
                    owner = slot // owned
                    low = (owner // 2) * owned * block + (slot % owned) * block
                    qt[owner % 2, low : low + block, at(n - GHOST - base)] = piece.T
            return 0

        lax.fori_loop(0, count, body, 0)

    for copy in copy_p[1:]:
        copy.wait()
    none = rows * kp
    spread(GHOST, GHOST, [*lower, *middle], p_own, none, True)
    spread(2 * GHOST, rows - 2 * GHOST, [*middle], p_own, none, True)
    spread(rows, GHOST, [*middle, *upper], p_own, none, True)
    copy_a.wait()

    def place(head, count, low, high):
        def body(i, _):
            g = head + i
            row = inner_row(g)
            local = [a_cols[k, 0, row] - (start - GHOST) for k in range(links)]
            for n in range(low, high):
                value = rows * links
                at_n = local_row(n)
                for k in range(links):
                    value = jnp.where(local[k] == at_n, row * links + k, value)
                piece = a_own[value]
                if n < GHOST:
                    dense_low[at(g), n * block : (n + 1) * block] = piece
                elif n < GHOST + rows:
                    dense[at(g), (n - GHOST) * block : (n - GHOST + 1) * block] = piece
                else:
                    m = n - GHOST - rows
                    dense_high[at(g - rows + GHOST), m * block : (m + 1) * block] = piece
            return 0

        lax.fori_loop(0, count, body, 0)

    place(0, GHOST, 0, GHOST + rows)
    place(GHOST, rows - 2 * GHOST, GHOST, GHOST + rows)
    place(rows - GHOST, GHOST, GHOST, rows + 2 * GHOST)

    gb = GHOST * block
    rb = rows * block
    bands = ((0, gb), (gb, rb - gb), (rb - gb, rb))
    inner = {0: (0, gb), 1: (0, rb), 2: (rb - gb, rb)}

    def own(band, c):
        head, last = bands[band]
        k0, k1 = inner[c]
        q, before = q_at[c]
        shift = gb - before * block
        keep = {(0, 0): 0, (0, 1): 1, (2, 1): 2, (2, 2): 3}.get((band, c))
        step = min(2 * block, last - head)
        for m in range(head, last, step):
            value = dot(dense[m : m + step, k0:k1], q[k0 + shift : k1 + shift, :])
            if keep is None:
                ap[c, m : m + step, :] = value.astype(bf)
            else:
                keep_ap[keep, m - head : m - head + step, :] = value

    def ghost(band, c):
        head, last = bands[band]
        q, before = q_at[c]
        left = dense_low if band == 0 else dense_high
        shift = (0 if band == 0 else gb + rb) - before * block
        keep = {(0, 0): 0, (0, 1): 1, (2, 1): 2, (2, 2): 3}[(band, c)]
        step = 2 * block
        for m in range(0, gb, step):
            value = dot(left[m : m + step, :], q[shift : shift + gb, :])
            ap[c, head + m : head + m + step, :] = (keep_ap[keep, m : m + step, :] + value).astype(bf)

    def stage_copy(t, j, c):
        return pltpu.make_async_remote_copy(
            src_ref=send_b[t].at[j, c], dst_ref=recv_b[t].at[j, c],
            send_sem=b_sem[t].at[j, c], recv_sem=b_got[t].at[j, c],
            device_id=(slab, partners[t]), device_id_type=MESH)

    quarters = 4
    slice_c = owned * block // quarters
    order = (2, 0, 1)

    def final_copy(o, c, h, relayed):
        piece = pl.ds(h * slice_c, slice_c)
        return pltpu.make_async_remote_copy(
            src_ref=send_c.at[o, c, piece], dst_ref=(pass_c.at[c, piece] if relayed else recv_c.at[o, c, piece]),
            send_sem=c_sem.at[o, c, h], recv_sem=(pass_c_got.at[c, h] if relayed else c_got.at[o, c, h]),
            device_id=(second if relayed else sides[o][2], me), device_id_type=MESH)

    def final_pass_copy(c, h):
        piece = pl.ds(h * slice_c, slice_c)
        return pltpu.make_async_remote_copy(
            src_ref=pass_c.at[c, piece], dst_ref=recv_c.at[0, c, piece],
            send_sem=pass_c_sem.at[c, h], recv_sem=c_got.at[0, c, h],
            device_id=(past, me), device_id_type=MESH)

    def final_through(k, c, h):
        return through(k, order.index(c) * quarters + h, chunks * quarters)

    def final_pass(c):
        for h in range(quarters):
            @pl.when(has_past & final_through(near, c, h))
            def _():
                final_copy(0, c, h, True).wait_recv()
                final_pass_copy(c, h).start()

    parts = ((qt0, 0, gb), (qt1, 0, rb), (qt2, rb - gb, gb))
    shape = (half, owned * block, edge)

    def form(j, c):
        qt, head, depth = parts[j]
        right = ap[c, head : head + depth, :]
        send_b[0][j, c] = dot(qt[1 - bits[0]], right).astype(bf).reshape(shape)
        stage_copy(0, j, c).start()
        keep_b[0][j, c] = dot(qt[bits[0]], right).reshape(shape)

    def fold(j, c):
        for t in range(1, stages):
            stage_copy(t - 1, j, c).wait_recv()
            for i in range(planes >> (t + 1)):
                k = 1 - bits[t] + 2 * i
                send_b[t][j, c, i] = (
                    keep_b[t - 1][j, c, k] + recv_b[t - 1][j, c, k].astype(f32)).astype(bf)
            stage_copy(t, j, c).start()
            for i in range(planes >> (t + 1)):
                k = bits[t] + 2 * i
                keep_b[t][j, c, i] = keep_b[t - 1][j, c, k] + recv_b[t - 1][j, c, k].astype(f32)

    def finish(j, c):
        stage_copy(stages - 1, j, c).wait_recv()
        value = keep_b[stages - 1][j, c, 0] + recv_b[stages - 1][j, c, 0].astype(f32)
        if j == 1:
            final[c] = value
        else:
            send_c[j // 2, c] = value.astype(bf)

    def send(j, c):
        o = j // 2
        exists = sides[o][3]
        for h in range(quarters):
            direct = exists
            if o == 0:
                direct = exists & ~final_through(far, c, h)

                @pl.when(exists & final_through(far, c, h))
                def _():
                    final_copy(o, c, h, True).start()

            @pl.when(direct)
            def _():
                final_copy(o, c, h, False).start()

    own(0, 2)
    form(0, 2)
    own(2, 0)
    form(2, 0)
    halo_pass(0)
    own(0, 0)
    own(0, 1)
    halo_pass(1)
    fold(0, 2)
    fold(2, 0)
    own(1, 1)
    halo_sent(0)
    halo_start(1)
    own(1, 0)
    own(1, 2)
    for i in range(2, GHOST - 1):
        halo_pass(i)
    own(2, 2)
    own(2, 1)
    halo_wait(0)
    spread(0, GHOST, [*lower, *middle], p_low, ghosts, False)
    ghost(0, 0)
    form(0, 0)
    ghost(0, 1)
    form(0, 1)
    finish(0, 2)
    finish(2, 0)
    fold(0, 0)
    fold(0, 1)
    form(1, 0)
    fold(1, 0)
    finish(0, 0)
    halo_sent(1)
    send(0, 2)
    send(0, 0)
    send(2, 0)
    halo_wait(1)
    spread(GHOST + rows, GHOST, [*middle, *upper], p_high, ghosts, False)
    ghost(2, 1)
    form(2, 1)
    ghost(2, 2)
    form(2, 2)
    finish(0, 1)
    send(0, 1)
    fold(2, 1)
    fold(2, 2)
    form(1, 2)
    fold(1, 2)
    form(1, 1)
    final_pass(2)
    fold(1, 1)
    final_pass(0)
    final_pass(1)
    finish(2, 1)
    send(2, 1)
    finish(2, 2)
    send(2, 2)
    finish(1, 0)
    finish(1, 2)
    finish(1, 1)

    def out_copy(o):
        column = jnp.where(turn == 0, o, 4 - o) * edge
        return pltpu.make_async_copy(whole.at[o], out.at[:, pl.ds(pl.multiple_of(column, edge), edge)], out_sem.at[o])

    for o in (0, 1, 2, 4, 3):
        terms = []
        if 0 <= o - 1 < chunks:
            terms.append(final[o - 1])
        for side, c in ((0, 2 - o), (1, 4 - o)):
            if 0 <= c < chunks:
                @pl.when(sides[side][3])
                def _():
                    for h in range(quarters):
                        final_copy(side, c, h, False).wait_recv()

                terms.append(recv_c[side, c].astype(f32))
        whole[o] = functools.reduce(jnp.add, terms)
        out_copy(o).start()

    for o in range(2):
        @pl.when(sides[o][3])
        def _():
            for c in range(chunks):
                for h in range(quarters):
                    final_copy(o, c, h, False).wait_send()

    for i in range(GHOST - 1):
        @pl.when(has_past & through(near, i, GHOST))
        def _():
            pass_copy(i).wait_send()

    for c in range(chunks):
        for h in range(quarters):
            @pl.when(has_past & final_through(near, c, h))
            def _():
                final_pass_copy(c, h).wait_send()

    for t in range(stages):
        for j in range(3):
            for c in range(chunks):
                stage_copy(t, j, c).wait_send()
    for o in range(5):
        out_copy(o).wait()


def on_device(a_blocks, a_cols, p_blocks, p_cols, coarse_slot):
    rows, links, block = a_blocks.shape[1:4]
    kp = p_blocks.shape[2]
    coarse = coarse_slot.shape[1]
    slabs = lax.axis_size("slab")
    planes = lax.axis_size("plane")
    owned = coarse // planes
    stages = planes.bit_length() - 1
    assert planes == 1 << stages and stages > 0 and rows >= 2 * GHOST
    edge = coarse * block
    high = owned * block
    dims = (slabs, planes, rows, links, kp, block, coarse, owned)
    bf, f32 = jnp.bfloat16, jnp.float32
    vmem = pltpu.VMEM
    dma = pltpu.SemaphoreType.DMA
    gb, rb = GHOST * block, rows * block
    shape = lambda t: (3, 3, planes >> (t + 1), high, edge)
    scratch = [
        vmem((rows * links + 1, block, block), bf),
        vmem((rows * kp + 1, block, block), bf),
        vmem((GHOST * kp + 1, block, block), bf),
        vmem((GHOST * kp + 1, block, block), bf),
        vmem((2 * gb, edge), bf),
        vmem((rb + 2 * gb, edge), bf),
        vmem((2 * gb, edge), bf),
        vmem((2, planes // 2 * high, gb), bf),
        vmem((2, planes // 2 * high, rb), bf),
        vmem((2, planes // 2 * high, gb), bf),
        vmem((rb, rb), bf),
        vmem((gb, gb), bf),
        vmem((gb, gb), bf),
        vmem((3, rb, edge), bf),
        vmem((4, gb, edge), f32),
        vmem((3, high, edge), f32),
        vmem((2, 3, high, edge), bf),
        vmem((2, 3, high, edge), bf),
        dma((4,)), dma((2, GHOST)), dma((2, GHOST)), dma((2, 3, 4)), dma((2, 3, 4)),
        vmem((5, high, edge), f32),
        dma((5,)),
        pltpu.SMEM((links, 1, rows), jnp.int32),
        pltpu.SMEM((planes, kp, p_cols.shape[1]), jnp.int32),
        pltpu.SMEM((coarse, slabs), jnp.int32),
        dma((3,)),
        vmem(((GHOST - 1) * kp, block, block), bf),
        vmem((3, high, edge), bf),
        dma((GHOST - 1,)), dma((GHOST - 1,)), dma((3, 4)), dma((3, 4)),
    ]
    scratch += [vmem(shape(t), bf) for t in range(stages)]
    scratch += [vmem(shape(t), bf) for t in range(stages)]
    scratch += [vmem(shape(t), f32) for t in range(stages)]
    scratch += [dma((3, 3)) for t in range(2 * stages)]
    outside = pl.BlockSpec(memory_space=pltpu.HBM)
    anywhere = pl.BlockSpec(memory_space=pl.ANY)
    result = pl.pallas_call(
        functools.partial(kernel, dims),
        out_shape=jax.ShapeDtypeStruct((high, 5 * edge), f32),
        in_specs=[outside] * 5,
        out_specs=anywhere,
        scratch_shapes=scratch,
        compiler_params=pltpu.CompilerParams(
            collective_id=0, has_side_effects=True, vmem_limit_bytes=50 * 1024 * 1024),
    )(*(pltpu.with_memory_space_constraint(x, pltpu.HBM) for x in (
        a_cols.transpose(2, 0, 1), p_cols.transpose(0, 2, 1), coarse_slot.T,
        a_blocks.reshape(rows * links, block, block), p_blocks.reshape(rows * kp, block, block))))
    return result.reshape(1, owned, block, 5 * edge)


def solution(mesh):
    return jax.shard_map(
        on_device,
        mesh=mesh,
        in_specs=(
            P("plane", "slab", None, None, None),
            P("plane", "slab", None),
            P("plane", "slab", None, None, None),
            P(),
            P(),
        ),
        out_specs=P("plane", "slab", None, None),
        check_vma=False,
    )
```

```python
import functools

import jax
import jax.numpy as jnp
from jax import lax
from jax.experimental import pallas as pl
from jax.experimental.pallas import tpu as pltpu
from jax.sharding import PartitionSpec as P

GHOST = 4
MESH = pl.DeviceIdType.MESH


def kernel(dims, a_cols_hbm, p_cols_hbm, slots_hbm, a_hbm, p_hbm, out, *scratch):
    slabs, planes, rows, links, kp, block, coarse, owned = dims
    stages = planes.bit_length() - 1
    edge = coarse * block
    chunks = 3
    ghosts = GHOST * kp
    (a_own, p_own, p_low, p_high, q0, q1, q2, qt0, qt1, qt2, dense, dense_low, dense_high, ap, keep_ap, final,
     send_c, recv_c, local_sem, halo_send, halo_recv, c_sem, c_got, a_cols, p_cols, slots,
     index_sem, pass_p, pass_c, pass_sem, pass_got, pass_c_sem, pass_c_got, table) = scratch[:34]
    rest = scratch[34:]
    send_b, recv_b, keep_b, b_sem, b_got = (rest[i * stages : (i + 1) * stages] for i in range(5))
    slab = lax.axis_index("slab")
    me = lax.axis_index("plane")
    bits = [(me // (1 << t)) % 2 for t in range(stages)]
    partners = [me + (1 - 2 * bits[t]) * (1 << t) for t in range(stages)]
    f32, bf = jnp.float32, jnp.bfloat16
    start = slab * rows
    total = p_cols.shape[2]
    dot = functools.partial(jnp.dot, preferred_element_type=f32)
    turn = slab % 2
    pairs = max(slabs // 2, 1)
    level = slab // 2
    first = slab - 1 + 2 * turn
    second = slab + 1 - 2 * turn
    past = slab + 2 - 4 * turn
    has_first = (first >= 0) & (first < slabs)
    has_second = second < slabs
    has_past = (past >= 0) & (past < slabs) & has_second
    far = jnp.where(has_second, jnp.where(turn == 0, level, pairs - 1 - level), 0)
    near = jnp.where(turn == 0, pairs - 1 - level, level)
    opening = turn * (rows - GHOST)
    closing = (1 - turn) * (rows - GHOST)

    def inner_row(i):
        return jnp.where(i < GHOST, opening + i, jnp.where(i < rows - GHOST, i, closing + i - (rows - GHOST)))

    def local_row(n):
        low = jnp.where(turn == 0, n, rows + GHOST + n)
        high = jnp.where(turn == 0, n, n - rows - GHOST)
        return jnp.where(n < GHOST, low, jnp.where(n < GHOST + rows, GHOST + inner_row(n - GHOST), high))

    copy_index = [
        pltpu.make_async_copy(source, target, index_sem.at[i])
        for i, (source, target) in enumerate(
            ((a_cols_hbm, a_cols), (p_cols_hbm, p_cols), (slots_hbm, slots)))
    ]
    spans = ((opening, GHOST), (closing, GHOST), (GHOST, rows - 2 * GHOST))
    copy_p = [
        pltpu.make_async_copy(
            p_hbm.at[pl.ds(head * kp, count * kp)], p_own.at[pl.ds(head * kp, count * kp)], local_sem.at[1 + i])
        for i, (head, count) in enumerate(spans)
    ]
    copy_a = pltpu.make_async_copy(a_hbm, a_own.at[pl.ds(0, rows * links)], local_sem.at[0])
    copy_p[0].start()
    for copy in copy_index:
        copy.start()
    for copy in copy_p[1:]:
        copy.start()
    copy_a.start()

    barrier = pltpu.get_barrier_semaphore()
    for t in range(stages):
        pl.semaphore_signal(barrier, inc=1, device_id=(slab, partners[t]), device_id_type=MESH)

    known = ((slab >= 1, slab - 1), (slab + 1 < slabs, slab + 1), (slab >= 2, slab - 2), (slab + 2 < slabs, slab + 2))
    for exists, device in known:
        @pl.when(exists)
        def _():
            pl.semaphore_signal(barrier, inc=1, device_id=(device, me), device_id_type=MESH)

    zero = jnp.zeros((block, block), bf)
    a_own[rows * links] = zero
    p_own[rows * kp] = zero
    p_low[ghosts] = zero
    p_high[ghosts] = zero

    @pl.when(~has_first)
    def _():
        p_low[...] = jnp.zeros_like(p_low)
        recv_c[0] = jnp.zeros(recv_c.shape[1:], recv_c.dtype)

    @pl.when(~has_second)
    def _():
        p_high[...] = jnp.zeros_like(p_high)
        recv_c[1] = jnp.zeros(recv_c.shape[1:], recv_c.dtype)

    pl.semaphore_wait(barrier, stages + sum(jnp.where(exists, 1, 0) for exists, _ in known))
    copy_p[0].wait()

    sides = ((opening, p_low, first, has_first), (closing, p_high, second, has_second))

    def through(k, i, units):
        return i < k * units // pairs

    units = 2 * GHOST
    early = units - 2
    piece_p = ghosts // units

    def row_copy(o, i, relayed):
        head, target, device, _ = sides[o]
        return pltpu.make_async_remote_copy(
            src_ref=p_own.at[pl.ds(head * kp + i * piece_p, piece_p)],
            dst_ref=(pass_p if relayed else target).at[pl.ds(i * piece_p, piece_p)],
            send_sem=halo_send.at[o, i], recv_sem=(pass_got.at[i] if relayed else halo_recv.at[o, i]),
            device_id=(second if relayed else device, me), device_id_type=MESH)

    def pass_copy(i):
        return pltpu.make_async_remote_copy(
            src_ref=pass_p.at[pl.ds(i * piece_p, piece_p)], dst_ref=p_low.at[pl.ds(i * piece_p, piece_p)],
            send_sem=pass_sem.at[i], recv_sem=halo_recv.at[0, i],
            device_id=(past, me), device_id_type=MESH)

    def halo_start(o):
        exists = sides[o][3]
        for i in range(units):
            direct = exists
            if o == 0 and i < units - 1:
                direct = exists & ~through(far, i, units)

                @pl.when(exists & through(far, i, units))
                def _():
                    row_copy(o, i, True).start()

            @pl.when(direct)
            def _():
                row_copy(o, i, False).start()

    def halo_sent(o, which):
        @pl.when(sides[o][3])
        def _():
            for i in which:
                row_copy(o, i, False).wait_send()

    def halo_pass(i, when=True):
        @pl.when(has_past & through(near, i, units) & when)
        def _():
            row_copy(0, i, True).wait_recv()
            pass_copy(i).start()

    most = 2 * near > pairs

    def halo_wait(o):
        @pl.when(sides[o][3])
        def _():
            for i in range(units):
                row_copy(o, i, False).wait_recv()

    halo_start(0)

    for copy in copy_index:
        copy.wait()

    def find(n, base, none, which):
        row = jnp.clip(start - GHOST + local_row(n), 0, total - 1)
        place = []
        for m in range(kp):
            col = p_cols[me, m, row]
            ahead = col // coarse
            place.append((1 + (ahead - slab) * (1 - 2 * turn)) * coarse + slots[col % coarse, ahead])
        found = []
        for w in which:
            value = none
            for m in range(kp):
                value = jnp.where(place[m] == w, base + m, value)
            found.append(value)
        return found

    def at(i):
        return pl.ds(pl.multiple_of(i * block, block), block)

    middle = range(coarse, 2 * coarse)
    lower = range(0, coarse)
    upper = range(2 * coarse, 3 * coarse)
    q_at = {0: (q0, 0), 1: (q1, 0), 2: (q2, rows)}
    turned = {0: (qt0, 0), 1: (qt1, 0), 2: (qt2, rows - GHOST)}
    half = planes // 2

    def chart(o, head, which):
        def body(i, _):
            for k, value in enumerate(find(head + i, i * kp, ghosts, which)):
                table[o, i, k] = value
            return 0

        lax.fori_loop(0, GHOST, body, 0)

    def spread(head, count, which, blocks, none, flip):
        def body(i, _):
            n = head + i
            if flip:
                found = find(n, inner_row(n - GHOST) * kp, none, which)
            else:
                found = [table[0 if head == 0 else 1, i, k] for k in range(len(which))]
            for w, value in zip(which, found):
                j, slot = w // coarse, w % coarse
                q, before = q_at[j]
                piece = blocks[value]
                q[at(n - before), slot * block : (slot + 1) * block] = piece
                if flip:
                    qt, base = turned[j]
                    owner = slot // owned
                    low = (owner // 2) * owned * block + (slot % owned) * block
                    qt[owner % 2, low : low + block, at(n - GHOST - base)] = piece.T
            return 0

        lax.fori_loop(0, count, body, 0)

    for copy in copy_p[1:]:
        copy.wait()
    none = rows * kp
    spread(GHOST, GHOST, [*lower, *middle], p_own, none, True)
    spread(2 * GHOST, rows - 2 * GHOST, [*middle], p_own, none, True)
    spread(rows, GHOST, [*middle, *upper], p_own, none, True)
    copy_a.wait()

    def place(head, count, low, high):
        def body(i, _):
            g = head + i
            row = inner_row(g)
            local = [a_cols[k, 0, row] - (start - GHOST) for k in range(links)]
            for n in range(low, high):
                value = rows * links
                at_n = local_row(n)
                for k in range(links):
                    value = jnp.where(local[k] == at_n, row * links + k, value)
                piece = a_own[value]
                if n < GHOST:
                    dense_low[at(g), n * block : (n + 1) * block] = piece
                elif n < GHOST + rows:
                    dense[at(g), (n - GHOST) * block : (n - GHOST + 1) * block] = piece
                else:
                    m = n - GHOST - rows
                    dense_high[at(g - rows + GHOST), m * block : (m + 1) * block] = piece
            return 0

        lax.fori_loop(0, count, body, 0)

    place(0, GHOST, 0, GHOST + rows)
    place(GHOST, rows - 2 * GHOST, GHOST, GHOST + rows)
    place(rows - GHOST, GHOST, GHOST, rows + 2 * GHOST)

    gb = GHOST * block
    rb = rows * block
    bands = ((0, gb), (gb, rb - gb), (rb - gb, rb))
    inner = {0: (0, gb), 1: (0, rb), 2: (rb - gb, rb)}

    def own(band, c):
        head, last = bands[band]
        k0, k1 = inner[c]
        q, before = q_at[c]
        shift = gb - before * block
        keep = {(0, 0): 0, (0, 1): 1, (2, 1): 2, (2, 2): 3}.get((band, c))
        step = min(2 * block, last - head)
        for m in range(head, last, step):
            value = dot(dense[m : m + step, k0:k1], q[k0 + shift : k1 + shift, :])
            if keep is None:
                ap[c, m : m + step, :] = value.astype(bf)
            else:
                keep_ap[keep, m - head : m - head + step, :] = value

    def ghost(band, c):
        head, last = bands[band]
        q, before = q_at[c]
        left = dense_low if band == 0 else dense_high
        shift = (0 if band == 0 else gb + rb) - before * block
        keep = {(0, 0): 0, (0, 1): 1, (2, 1): 2, (2, 2): 3}[(band, c)]
        step = 2 * block
        for m in range(0, gb, step):
            value = dot(left[m : m + step, :], q[shift : shift + gb, :])
            ap[c, head + m : head + m + step, :] = (keep_ap[keep, m : m + step, :] + value).astype(bf)

    def stage_copy(t, j, c):
        return pltpu.make_async_remote_copy(
            src_ref=send_b[t].at[j, c], dst_ref=recv_b[t].at[j, c],
            send_sem=b_sem[t].at[j, c], recv_sem=b_got[t].at[j, c],
            device_id=(slab, partners[t]), device_id_type=MESH)

    quarters = 4
    slice_c = owned * block // quarters
    order = (2, 0, 1)

    def final_copy(o, c, h, relayed):
        piece = pl.ds(h * slice_c, slice_c)
        return pltpu.make_async_remote_copy(
            src_ref=send_c.at[o, c, piece], dst_ref=(pass_c.at[c, piece] if relayed else recv_c.at[o, c, piece]),
            send_sem=c_sem.at[o, c, h], recv_sem=(pass_c_got.at[c, h] if relayed else c_got.at[o, c, h]),
            device_id=(second if relayed else sides[o][2], me), device_id_type=MESH)

    def final_pass_copy(c, h):
        piece = pl.ds(h * slice_c, slice_c)
        return pltpu.make_async_remote_copy(
            src_ref=pass_c.at[c, piece], dst_ref=recv_c.at[0, c, piece],
            send_sem=pass_c_sem.at[c, h], recv_sem=c_got.at[0, c, h],
            device_id=(past, me), device_id_type=MESH)

    def final_through(k, c, h):
        return through(k, order.index(c) * quarters + h, chunks * quarters) & (c != order[-1])

    def final_pass(c):
        for h in range(quarters):
            @pl.when(has_past & final_through(near, c, h))
            def _():
                final_copy(0, c, h, True).wait_recv()
                final_pass_copy(c, h).start()

    parts = ((qt0, 0, gb), (qt1, 0, rb), (qt2, rb - gb, gb))
    shape = (half, owned * block, edge)

    def form(j, c):
        qt, head, depth = parts[j]
        right = ap[c, head : head + depth, :]
        send_b[0][j, c] = dot(qt[1 - bits[0]], right).astype(bf).reshape(shape)
        stage_copy(0, j, c).start()
        keep_b[0][j, c] = dot(qt[bits[0]], right).reshape(shape)

    def fold(j, c):
        for t in range(1, stages):
            stage_copy(t - 1, j, c).wait_recv()
            for i in range(planes >> (t + 1)):
                k = 1 - bits[t] + 2 * i
                send_b[t][j, c, i] = (
                    keep_b[t - 1][j, c, k] + recv_b[t - 1][j, c, k].astype(f32)).astype(bf)
            stage_copy(t, j, c).start()
            for i in range(planes >> (t + 1)):
                k = bits[t] + 2 * i
                keep_b[t][j, c, i] = keep_b[t - 1][j, c, k] + recv_b[t - 1][j, c, k].astype(f32)

    def finish(j, c):
        stage_copy(stages - 1, j, c).wait_recv()
        value = keep_b[stages - 1][j, c, 0] + recv_b[stages - 1][j, c, 0].astype(f32)
        if j == 1:
            final[c] = value
        else:
            send_c[j // 2, c] = value.astype(bf)

    def send(j, c):
        o = j // 2
        exists = sides[o][3]
        for h in range(quarters):
            direct = exists
            if o == 0:
                direct = exists & ~final_through(far, c, h)

                @pl.when(exists & final_through(far, c, h))
                def _():
                    final_copy(o, c, h, True).start()

            @pl.when(direct)
            def _():
                final_copy(o, c, h, False).start()

    def write(o):
        terms = []
        if 0 <= o - 1 < chunks:
            terms.append(final[o - 1])
        for side, c in ((0, 2 - o), (1, 4 - o)):
            if 0 <= c < chunks:
                @pl.when(sides[side][3])
                def _():
                    for h in range(quarters):
                        final_copy(side, c, h, False).wait_recv()

                terms.append(recv_c[side, c].astype(f32))
        column = jnp.where(turn == 0, o, 4 - o) * edge
        out[:, pl.ds(pl.multiple_of(column, edge), edge)] = functools.reduce(jnp.add, terms)

    own(0, 2)
    form(0, 2)
    own(2, 0)
    form(2, 0)
    halo_pass(0, most)
    own(0, 0)
    halo_pass(0, ~most)
    own(0, 1)
    halo_pass(1, most)
    fold(0, 2)
    fold(2, 0)
    own(1, 0)
    own(1, 2)
    halo_pass(2, most)
    own(1, 1)
    halo_pass(3, most)
    halo_sent(0, range(early))
    halo_start(1)
    halo_pass(1, ~most)
    own(2, 2)
    own(2, 1)
    halo_pass(4, most)
    chart(0, 0, [*lower, *middle])
    halo_pass(2, ~most)
    halo_pass(3, ~most)
    halo_pass(4, ~most)
    for i in range(5, units - 1):
        halo_pass(i)
    halo_wait(0)
    spread(0, GHOST, [*lower, *middle], p_low, ghosts, False)
    ghost(0, 0)
    form(0, 0)
    ghost(0, 1)
    form(0, 1)
    finish(0, 2)
    finish(2, 0)
    fold(0, 0)
    fold(0, 1)
    form(1, 0)
    fold(1, 0)
    chart(1, GHOST + rows, [*middle, *upper])
    halo_sent(0, range(early, units))
    halo_sent(1, range(units))
    send(0, 2)
    send(2, 0)
    finish(0, 0)
    send(0, 0)
    halo_wait(1)
    spread(GHOST + rows, GHOST, [*middle, *upper], p_high, ghosts, False)
    ghost(2, 1)
    form(2, 1)
    ghost(2, 2)
    form(2, 2)
    fold(2, 1)
    finish(0, 1)
    send(0, 1)
    fold(2, 2)
    form(1, 2)
    fold(1, 2)
    form(1, 1)
    final_pass(2)
    fold(1, 1)
    finish(2, 1)
    send(2, 1)
    final_pass(0)
    finish(2, 2)
    send(2, 2)
    finish(1, 0)
    write(0)
    write(1)
    write(4)
    finish(1, 2)
    finish(1, 1)
    write(3)
    write(2)

    for o in range(2):
        @pl.when(sides[o][3])
        def _():
            for c in range(chunks):
                for h in range(quarters):
                    final_copy(o, c, h, False).wait_send()

    for i in range(units - 1):
        @pl.when(has_past & through(near, i, units))
        def _():
            pass_copy(i).wait_send()

    for c in range(chunks):
        for h in range(quarters):
            @pl.when(has_past & final_through(near, c, h))
            def _():
                final_pass_copy(c, h).wait_send()

    for t in range(stages):
        for j in range(3):
            for c in range(chunks):
                stage_copy(t, j, c).wait_send()


def on_device(a_blocks, a_cols, p_blocks, p_cols, coarse_slot):
    rows, links, block = a_blocks.shape[1:4]
    kp = p_blocks.shape[2]
    coarse = coarse_slot.shape[1]
    slabs = lax.axis_size("slab")
    planes = lax.axis_size("plane")
    owned = coarse // planes
    stages = planes.bit_length() - 1
    assert planes == 1 << stages and stages > 0 and rows >= 2 * GHOST
    edge = coarse * block
    high = owned * block
    dims = (slabs, planes, rows, links, kp, block, coarse, owned)
    bf, f32 = jnp.bfloat16, jnp.float32
    vmem = pltpu.VMEM
    dma = pltpu.SemaphoreType.DMA
    gb, rb = GHOST * block, rows * block
    shape = lambda t: (3, 3, planes >> (t + 1), high, edge)
    scratch = [
        vmem((rows * links + 1, block, block), bf),
        vmem((rows * kp + 1, block, block), bf),
        vmem((GHOST * kp + 1, block, block), bf),
        vmem((GHOST * kp + 1, block, block), bf),
        vmem((2 * gb, edge), bf),
        vmem((rb + 2 * gb, edge), bf),
        vmem((2 * gb, edge), bf),
        vmem((2, planes // 2 * high, gb), bf),
        vmem((2, planes // 2 * high, rb), bf),
        vmem((2, planes // 2 * high, gb), bf),
        vmem((rb, rb), bf),
        vmem((gb, gb), bf),
        vmem((gb, gb), bf),
        vmem((3, rb, edge), bf),
        vmem((4, gb, edge), f32),
        vmem((3, high, edge), f32),
        vmem((2, 3, high, edge), bf),
        vmem((2, 3, high, edge), bf),
        dma((4,)), dma((2, 2 * GHOST)), dma((2, 2 * GHOST)), dma((2, 3, 4)), dma((2, 3, 4)),
        pltpu.SMEM((links, 1, rows), jnp.int32),
        pltpu.SMEM((planes, kp, p_cols.shape[1]), jnp.int32),
        pltpu.SMEM((coarse, slabs), jnp.int32),
        dma((3,)),
        vmem((GHOST * kp, block, block), bf),
        vmem((3, high, edge), bf),
        dma((2 * GHOST,)), dma((2 * GHOST,)), dma((3, 4)), dma((3, 4)),
        pltpu.SMEM((2, GHOST, 2 * coarse), jnp.int32),
    ]
    scratch += [vmem(shape(t), bf) for t in range(stages)]
    scratch += [vmem(shape(t), bf) for t in range(stages)]
    scratch += [vmem(shape(t), f32) for t in range(stages)]
    scratch += [dma((3, 3)) for t in range(2 * stages)]
    outside = pl.BlockSpec(memory_space=pltpu.HBM)
    result = pl.pallas_call(
        functools.partial(kernel, dims),
        out_shape=jax.ShapeDtypeStruct((high, 5 * edge), f32),
        in_specs=[outside] * 5,
        out_specs=pl.BlockSpec(memory_space=pltpu.VMEM),
        scratch_shapes=scratch,
        compiler_params=pltpu.CompilerParams(
            collective_id=0, has_side_effects=True, vmem_limit_bytes=50 * 1024 * 1024),
    )(*(pltpu.with_memory_space_constraint(x, pltpu.HBM) for x in (
        a_cols.transpose(2, 0, 1), p_cols.transpose(0, 2, 1), coarse_slot.T,
        a_blocks.reshape(rows * links, block, block), p_blocks.reshape(rows * kp, block, block))))
    return result.reshape(1, owned, block, 5 * edge)


def solution(mesh):
    return jax.shard_map(
        on_device,
        mesh=mesh,
        in_specs=(
            P("plane", "slab", None, None, None),
            P("plane", "slab", None),
            P("plane", "slab", None, None, None),
            P(),
            P(),
        ),
        out_specs=P("plane", "slab", None, None),
        check_vma=False,
    )
```

```python
import functools

import jax
import jax.numpy as jnp
from jax import lax
from jax.experimental import pallas as pl
from jax.experimental.pallas import tpu as pltpu
from jax.sharding import PartitionSpec as P

GHOST = 4
MESH = pl.DeviceIdType.MESH


def kernel(dims, a_cols_hbm, p_cols_hbm, slots_hbm, a_hbm, p_hbm, out, *scratch):
    slabs, planes, rows, links, kp, block, coarse, owned = dims
    stages = planes.bit_length() - 1
    edge = coarse * block
    chunks = 3
    ghosts = GHOST * kp
    (a_own, p_own, p_low, p_high, q0, q1, q2, qt0, qt1, qt2, dense, dense_low, dense_high, ap, keep_ap, final,
     send_c, recv_c, local_sem, halo_send, halo_recv, c_sem, c_got, a_cols, p_cols, slots,
     index_sem, pass_p, pass_c, pass_sem, pass_got, pass_c_sem, pass_c_got, table) = scratch[:34]
    rest = scratch[34:]
    send_b, recv_b, keep_b, b_sem, b_got = (rest[i * stages : (i + 1) * stages] for i in range(5))
    slab = lax.axis_index("slab")
    me = lax.axis_index("plane")
    bits = [(me // (1 << t)) % 2 for t in range(stages)]
    partners = [me + (1 - 2 * bits[t]) * (1 << t) for t in range(stages)]
    f32, bf = jnp.float32, jnp.bfloat16
    start = slab * rows
    total = p_cols.shape[2]
    dot = functools.partial(jnp.dot, preferred_element_type=f32)
    turn = slab % 2
    pairs = max(slabs // 2, 1)
    level = slab // 2
    first = slab - 1 + 2 * turn
    second = slab + 1 - 2 * turn
    past = slab + 2 - 4 * turn
    has_first = (first >= 0) & (first < slabs)
    has_second = second < slabs
    has_past = (past >= 0) & (past < slabs) & has_second
    far = jnp.where(has_second, jnp.where(turn == 0, level, pairs - 1 - level), 0)
    near = jnp.where(turn == 0, pairs - 1 - level, level)
    opening = turn * (rows - GHOST)
    closing = (1 - turn) * (rows - GHOST)

    def inner_row(i):
        return jnp.where(i < GHOST, opening + i, jnp.where(i < rows - GHOST, i, closing + i - (rows - GHOST)))

    def local_row(n):
        low = jnp.where(turn == 0, n, rows + GHOST + n)
        high = jnp.where(turn == 0, n, n - rows - GHOST)
        return jnp.where(n < GHOST, low, jnp.where(n < GHOST + rows, GHOST + inner_row(n - GHOST), high))

    copy_index = [
        pltpu.make_async_copy(source, target, index_sem.at[i])
        for i, (source, target) in enumerate(
            ((a_cols_hbm, a_cols), (p_cols_hbm, p_cols), (slots_hbm, slots)))
    ]
    spans = ((opening, GHOST), (closing, GHOST), (GHOST, rows - 2 * GHOST))
    copy_p = [
        pltpu.make_async_copy(
            p_hbm.at[pl.ds(head * kp, count * kp)], p_own.at[pl.ds(head * kp, count * kp)], local_sem.at[1 + i])
        for i, (head, count) in enumerate(spans)
    ]
    copy_a = pltpu.make_async_copy(a_hbm, a_own.at[pl.ds(0, rows * links)], local_sem.at[0])
    copy_p[0].start()
    for copy in copy_index:
        copy.start()
    for copy in copy_p[1:]:
        copy.start()
    copy_a.start()

    barrier = pltpu.get_barrier_semaphore()
    for t in range(stages):
        pl.semaphore_signal(barrier, inc=1, device_id=(slab, partners[t]), device_id_type=MESH)

    known = ((slab >= 1, slab - 1), (slab + 1 < slabs, slab + 1), (slab >= 2, slab - 2), (slab + 2 < slabs, slab + 2))
    for exists, device in known:
        @pl.when(exists)
        def _():
            pl.semaphore_signal(barrier, inc=1, device_id=(device, me), device_id_type=MESH)

    zero = jnp.zeros((block, block), bf)
    a_own[rows * links] = zero
    p_own[rows * kp] = zero
    p_low[ghosts] = zero
    p_high[ghosts] = zero

    @pl.when(~has_first)
    def _():
        p_low[...] = jnp.zeros_like(p_low)
        recv_c[0] = jnp.zeros(recv_c.shape[1:], recv_c.dtype)

    @pl.when(~has_second)
    def _():
        p_high[...] = jnp.zeros_like(p_high)
        recv_c[1] = jnp.zeros(recv_c.shape[1:], recv_c.dtype)

    pl.semaphore_wait(barrier, stages + sum(jnp.where(exists, 1, 0) for exists, _ in known))
    copy_p[0].wait()

    sides = ((opening, p_low, first, has_first), (closing, p_high, second, has_second))

    def through(k, i, units):
        return i < k * units // pairs

    units = 2 * GHOST
    early = units - 2
    piece_p = ghosts // units

    def row_copy(o, i, relayed):
        head, target, device, _ = sides[o]
        return pltpu.make_async_remote_copy(
            src_ref=p_own.at[pl.ds(head * kp + i * piece_p, piece_p)],
            dst_ref=(pass_p if relayed else target).at[pl.ds(i * piece_p, piece_p)],
            send_sem=halo_send.at[o, i], recv_sem=(pass_got.at[i] if relayed else halo_recv.at[o, i]),
            device_id=(second if relayed else device, me), device_id_type=MESH)

    def pass_copy(i):
        return pltpu.make_async_remote_copy(
            src_ref=pass_p.at[pl.ds(i * piece_p, piece_p)], dst_ref=p_low.at[pl.ds(i * piece_p, piece_p)],
            send_sem=pass_sem.at[i], recv_sem=halo_recv.at[0, i],
            device_id=(past, me), device_id_type=MESH)

    def halo_start(o):
        exists = sides[o][3]
        for i in range(units):
            direct = exists
            if o == 0 and i < units - 1:
                direct = exists & ~through(far, i, units)

                @pl.when(exists & through(far, i, units))
                def _():
                    row_copy(o, i, True).start()

            @pl.when(direct)
            def _():
                row_copy(o, i, False).start()

    def halo_sent(o, which):
        @pl.when(sides[o][3])
        def _():
            for i in which:
                row_copy(o, i, False).wait_send()

    def halo_pass(i, when=True):
        @pl.when(has_past & through(near, i, units) & when)
        def _():
            row_copy(0, i, True).wait_recv()
            pass_copy(i).start()

    most = 2 * near > pairs

    def halo_wait(o):
        @pl.when(sides[o][3])
        def _():
            for i in range(units):
                row_copy(o, i, False).wait_recv()

    halo_start(0)

    for copy in copy_index:
        copy.wait()

    def find(n, base, none, which):
        row = jnp.clip(start - GHOST + local_row(n), 0, total - 1)
        place = []
        for m in range(kp):
            col = p_cols[me, m, row]
            ahead = col // coarse
            place.append((1 + (ahead - slab) * (1 - 2 * turn)) * coarse + slots[col % coarse, ahead])
        found = []
        for w in which:
            value = none
            for m in range(kp):
                value = jnp.where(place[m] == w, base + m, value)
            found.append(value)
        return found

    def at(i):
        return pl.ds(pl.multiple_of(i * block, block), block)

    middle = range(coarse, 2 * coarse)
    lower = range(0, coarse)
    upper = range(2 * coarse, 3 * coarse)
    q_at = {0: (q0, 0), 1: (q1, 0), 2: (q2, rows)}
    turned = {0: (qt0, 0), 1: (qt1, 0), 2: (qt2, rows - GHOST)}
    half = planes // 2

    def chart(o, head, which):
        def body(i, _):
            for k, value in enumerate(find(head + i, i * kp, ghosts, which)):
                table[o, i, k] = value
            return 0

        lax.fori_loop(0, GHOST, body, 0)

    def spread(head, count, which, blocks, none, flip):
        def body(i, _):
            n = head + i
            if flip:
                found = find(n, inner_row(n - GHOST) * kp, none, which)
            else:
                found = [table[0 if head == 0 else 1, i, k] for k in range(len(which))]
            for w, value in zip(which, found):
                j, slot = w // coarse, w % coarse
                q, before = q_at[j]
                piece = blocks[value]
                q[at(n - before), slot * block : (slot + 1) * block] = piece
                if flip:
                    qt, base = turned[j]
                    owner = slot // owned
                    low = (owner // 2) * owned * block + (slot % owned) * block
                    qt[owner % 2, low : low + block, at(n - GHOST - base)] = piece.T
            return 0

        lax.fori_loop(0, count, body, 0)

    for copy in copy_p[1:]:
        copy.wait()
    none = rows * kp
    spread(GHOST, GHOST, [*lower, *middle], p_own, none, True)
    spread(2 * GHOST, rows - 2 * GHOST, [*middle], p_own, none, True)
    spread(rows, GHOST, [*middle, *upper], p_own, none, True)
    copy_a.wait()

    def place(head, count, low, high):
        def body(i, _):
            g = head + i
            row = inner_row(g)
            local = [a_cols[k, 0, row] - (start - GHOST) for k in range(links)]
            for n in range(low, high):
                value = rows * links
                at_n = local_row(n)
                for k in range(links):
                    value = jnp.where(local[k] == at_n, row * links + k, value)
                piece = a_own[value]
                if n < GHOST:
                    dense_low[at(g), n * block : (n + 1) * block] = piece
                elif n < GHOST + rows:
                    dense[at(g), (n - GHOST) * block : (n - GHOST + 1) * block] = piece
                else:
                    m = n - GHOST - rows
                    dense_high[at(g - rows + GHOST), m * block : (m + 1) * block] = piece
            return 0

        lax.fori_loop(0, count, body, 0)

    place(0, GHOST, 0, GHOST + rows)
    place(GHOST, rows - 2 * GHOST, GHOST, GHOST + rows)
    place(rows - GHOST, GHOST, GHOST, rows + 2 * GHOST)

    gb = GHOST * block
    rb = rows * block
    bands = ((0, gb), (gb, rb - gb), (rb - gb, rb))
    inner = {0: (0, gb), 1: (0, rb), 2: (rb - gb, rb)}

    def own(band, c):
        head, last = bands[band]
        k0, k1 = inner[c]
        q, before = q_at[c]
        shift = gb - before * block
        keep = {(0, 0): 0, (0, 1): 1, (2, 1): 2, (2, 2): 3}.get((band, c))
        step = min(2 * block, last - head)
        for m in range(head, last, step):
            value = dot(dense[m : m + step, k0:k1], q[k0 + shift : k1 + shift, :])
            if keep is None:
                ap[c, m : m + step, :] = value.astype(bf)
            else:
                keep_ap[keep, m - head : m - head + step, :] = value

    def ghost(band, c):
        head, last = bands[band]
        q, before = q_at[c]
        left = dense_low if band == 0 else dense_high
        shift = (0 if band == 0 else gb + rb) - before * block
        keep = {(0, 0): 0, (0, 1): 1, (2, 1): 2, (2, 2): 3}[(band, c)]
        step = 2 * block
        for m in range(0, gb, step):
            value = dot(left[m : m + step, :], q[shift : shift + gb, :])
            ap[c, head + m : head + m + step, :] = (keep_ap[keep, m : m + step, :] + value).astype(bf)

    def stage_copy(t, j, c, k):
        return pltpu.make_async_remote_copy(
            src_ref=send_b[t].at[j, c, k], dst_ref=recv_b[t].at[j, c, k],
            send_sem=b_sem[t].at[j, c, k], recv_sem=b_got[t].at[j, c, k],
            device_id=(slab, partners[t]), device_id_type=MESH)

    quarters = 4
    slice_c = owned * block // quarters
    order = (2, 0, 1)

    def final_copy(o, c, h, relayed):
        piece = pl.ds(h * slice_c, slice_c)
        return pltpu.make_async_remote_copy(
            src_ref=send_c.at[o, c, piece], dst_ref=(pass_c.at[c, piece] if relayed else recv_c.at[o, c, piece]),
            send_sem=c_sem.at[o, c, h], recv_sem=(pass_c_got.at[c, h] if relayed else c_got.at[o, c, h]),
            device_id=(second if relayed else sides[o][2], me), device_id_type=MESH)

    def final_pass_copy(c, h):
        piece = pl.ds(h * slice_c, slice_c)
        return pltpu.make_async_remote_copy(
            src_ref=pass_c.at[c, piece], dst_ref=recv_c.at[0, c, piece],
            send_sem=pass_c_sem.at[c, h], recv_sem=c_got.at[0, c, h],
            device_id=(past, me), device_id_type=MESH)

    def final_through(k, c, h):
        return through(k, order.index(c) * quarters + h, chunks * quarters) & (c != order[-1])

    def final_pass(c):
        for h in range(quarters):
            @pl.when(has_past & final_through(near, c, h))
            def _():
                final_copy(0, c, h, True).wait_recv()
                final_pass_copy(c, h).start()

    parts = ((qt0, 0, gb), (qt1, 0, rb), (qt2, rb - gb, gb))
    shape = (half, owned * block, edge)

    tall = owned * block
    picks = [1 - bits[1] + 2 * i for i in range(half // 2)] + [bits[1] + 2 * i for i in range(half // 2)]

    def form(j, c):
        qt, head, depth = parts[j]
        right = ap[c, head : head + depth, :]
        send_b[0][j, c] = dot(qt[1 - bits[0]], right).astype(bf).reshape(shape)
        for k in picks:
            stage_copy(0, j, c, k).start()
        keep_b[0][j, c] = dot(qt[bits[0]], right).reshape(shape)

    def fold(j, c):
        for t in range(1, stages):
            for i in range(planes >> (t + 1)):
                k = 1 - bits[t] + 2 * i
                stage_copy(t - 1, j, c, k).wait_recv()
                send_b[t][j, c, i] = (
                    keep_b[t - 1][j, c, k] + recv_b[t - 1][j, c, k].astype(f32)).astype(bf)
                stage_copy(t, j, c, i).start()
            for i in range(planes >> (t + 1)):
                k = bits[t] + 2 * i
                stage_copy(t - 1, j, c, k).wait_recv()
                keep_b[t][j, c, i] = keep_b[t - 1][j, c, k] + recv_b[t - 1][j, c, k].astype(f32)

    def finish(j, c):
        stage_copy(stages - 1, j, c, 0).wait_recv()
        value = keep_b[stages - 1][j, c, 0] + recv_b[stages - 1][j, c, 0].astype(f32)
        if j == 1:
            final[c] = value
        else:
            send_c[j // 2, c] = value.astype(bf)

    def send(j, c):
        o = j // 2
        exists = sides[o][3]
        for h in range(quarters):
            direct = exists
            if o == 0:
                direct = exists & ~final_through(far, c, h)

                @pl.when(exists & final_through(far, c, h))
                def _():
                    final_copy(o, c, h, True).start()

            @pl.when(direct)
            def _():
                final_copy(o, c, h, False).start()

    def write(o):
        terms = []
        if 0 <= o - 1 < chunks:
            terms.append(final[o - 1])
        for side, c in ((0, 2 - o), (1, 4 - o)):
            if 0 <= c < chunks:
                @pl.when(sides[side][3])
                def _():
                    for h in range(quarters):
                        final_copy(side, c, h, False).wait_recv()

                terms.append(recv_c[side, c].astype(f32))
        column = jnp.where(turn == 0, o, 4 - o) * edge
        out[:, pl.ds(pl.multiple_of(column, edge), edge)] = functools.reduce(jnp.add, terms)

    own(0, 2)
    form(0, 2)
    halo_pass(0, most)
    own(2, 0)
    form(2, 0)
    halo_pass(1, most)
    halo_pass(0, ~most)
    own(0, 0)
    own(0, 1)
    halo_pass(2, most)
    fold(0, 2)
    fold(2, 0)
    own(1, 0)
    halo_pass(3, most)
    halo_pass(1, ~most)
    halo_sent(0, range(early))
    halo_start(1)
    own(1, 2)
    own(1, 1)
    halo_pass(4, most)
    halo_pass(2, ~most)
    own(2, 2)
    own(2, 1)
    chart(0, 0, [*lower, *middle])
    halo_pass(3, ~most)
    halo_pass(4, ~most)
    for i in range(5, units - 1):
        halo_pass(i)
    halo_wait(0)
    spread(0, GHOST, [*lower, *middle], p_low, ghosts, False)
    ghost(0, 0)
    form(0, 0)
    ghost(0, 1)
    form(0, 1)
    finish(0, 2)
    finish(2, 0)
    fold(0, 0)
    fold(0, 1)
    form(1, 0)
    fold(1, 0)
    chart(1, GHOST + rows, [*middle, *upper])
    halo_sent(0, range(early, units))
    halo_sent(1, range(units))
    send(0, 2)
    send(2, 0)
    finish(0, 0)
    send(0, 0)
    halo_wait(1)
    spread(GHOST + rows, GHOST, [*middle, *upper], p_high, ghosts, False)
    ghost(2, 1)
    form(2, 1)
    ghost(2, 2)
    form(2, 2)
    fold(2, 1)
    finish(0, 1)
    send(0, 1)
    fold(2, 2)
    form(1, 2)
    fold(1, 2)
    form(1, 1)
    final_pass(2)
    fold(1, 1)
    finish(2, 1)
    send(2, 1)
    final_pass(0)
    finish(2, 2)
    send(2, 2)
    finish(1, 0)
    write(0)
    write(1)
    write(4)
    finish(1, 2)
    finish(1, 1)
    write(3)
    write(2)

    for o in range(2):
        @pl.when(sides[o][3])
        def _():
            for c in range(chunks):
                for h in range(quarters):
                    final_copy(o, c, h, False).wait_send()

    for i in range(units - 1):
        @pl.when(has_past & through(near, i, units))
        def _():
            pass_copy(i).wait_send()

    for c in range(chunks):
        for h in range(quarters):
            @pl.when(has_past & final_through(near, c, h))
            def _():
                final_pass_copy(c, h).wait_send()

    for t in range(stages):
        for j in range(3):
            for c in range(chunks):
                for k in range(planes >> (t + 1)):
                    stage_copy(t, j, c, k).wait_send()


def on_device(a_blocks, a_cols, p_blocks, p_cols, coarse_slot):
    rows, links, block = a_blocks.shape[1:4]
    kp = p_blocks.shape[2]
    coarse = coarse_slot.shape[1]
    slabs = lax.axis_size("slab")
    planes = lax.axis_size("plane")
    owned = coarse // planes
    stages = planes.bit_length() - 1
    assert planes == 1 << stages and stages > 1 and rows >= 2 * GHOST
    edge = coarse * block
    high = owned * block
    dims = (slabs, planes, rows, links, kp, block, coarse, owned)
    bf, f32 = jnp.bfloat16, jnp.float32
    vmem = pltpu.VMEM
    dma = pltpu.SemaphoreType.DMA
    gb, rb = GHOST * block, rows * block
    shape = lambda t: (3, 3, planes >> (t + 1), high, edge)
    scratch = [
        vmem((rows * links + 1, block, block), bf),
        vmem((rows * kp + 1, block, block), bf),
        vmem((GHOST * kp + 1, block, block), bf),
        vmem((GHOST * kp + 1, block, block), bf),
        vmem((2 * gb, edge), bf),
        vmem((rb + 2 * gb, edge), bf),
        vmem((2 * gb, edge), bf),
        vmem((2, planes // 2 * high, gb), bf),
        vmem((2, planes // 2 * high, rb), bf),
        vmem((2, planes // 2 * high, gb), bf),
        vmem((rb, rb), bf),
        vmem((gb, gb), bf),
        vmem((gb, gb), bf),
        vmem((3, rb, edge), bf),
        vmem((4, gb, edge), f32),
        vmem((3, high, edge), f32),
        vmem((2, 3, high, edge), bf),
        vmem((2, 3, high, edge), bf),
        dma((4,)), dma((2, 2 * GHOST)), dma((2, 2 * GHOST)), dma((2, 3, 4)), dma((2, 3, 4)),
        pltpu.SMEM((links, 1, rows), jnp.int32),
        pltpu.SMEM((planes, kp, p_cols.shape[1]), jnp.int32),
        pltpu.SMEM((coarse, slabs), jnp.int32),
        dma((3,)),
        vmem((GHOST * kp, block, block), bf),
        vmem((3, high, edge), bf),
        dma((2 * GHOST,)), dma((2 * GHOST,)), dma((3, 4)), dma((3, 4)),
        pltpu.SMEM((2, GHOST, 2 * coarse), jnp.int32),
    ]
    scratch += [vmem(shape(t), bf) for t in range(stages)]
    scratch += [vmem(shape(t), bf) for t in range(stages)]
    scratch += [vmem(shape(t), f32) for t in range(stages)]
    scratch += [dma(shape(t % stages)[:3]) for t in range(2 * stages)]
    outside = pl.BlockSpec(memory_space=pltpu.HBM)
    result = pl.pallas_call(
        functools.partial(kernel, dims),
        out_shape=jax.ShapeDtypeStruct((high, 5 * edge), f32),
        in_specs=[outside] * 5,
        out_specs=pl.BlockSpec(memory_space=pltpu.VMEM),
        scratch_shapes=scratch,
        compiler_params=pltpu.CompilerParams(
            collective_id=0, has_side_effects=True, vmem_limit_bytes=50 * 1024 * 1024),
    )(*(pltpu.with_memory_space_constraint(x, pltpu.HBM) for x in (
        a_cols.transpose(2, 0, 1), p_cols.transpose(0, 2, 1), coarse_slot.T,
        a_blocks.reshape(rows * links, block, block), p_blocks.reshape(rows * kp, block, block))))
    return result.reshape(1, owned, block, 5 * edge)


def solution(mesh):
    return jax.shard_map(
        on_device,
        mesh=mesh,
        in_specs=(
            P("plane", "slab", None, None, None),
            P("plane", "slab", None),
            P("plane", "slab", None, None, None),
            P(),
            P(),
        ),
        out_specs=P("plane", "slab", None, None),
        check_vma=False,
    )
```
